16 devices in a mesh: sweep: 2 (over y, z), ent: 8 (over x, core).
Axes of the slice: x: 4, y: 2, z: 1, core: 2. Of those that a mesh axis runs over, the one named last changes fastest.
The devices are a block of a 4x4x8 slice.
Arguments:
- ent_table: float32 [65536, 200], P(('sweep', 'ent')), parts along dimension 0
- ent_accum: float32 [65536], P(('sweep', 'ent')), parts along dimension 0
- rel_table: float32 [22, 200], P('sweep'), parts along dimension 0
- rel_accum: float32 [22], P('sweep'), parts along dimension 0
- head_idx: int32 [16, 8, 2048], P(('sweep', 'ent')), parts along dimension 0
- tail_idx: int32 [16, 8, 2048], P(('sweep', 'ent')), parts along dimension 0
- rel_idx: int32 [16, 8, 2048], P(('sweep', 'ent')), parts along dimension 0
- edge_mask: int32 [16, 8, 2048], P(('sweep', 'ent')), parts along dimension 0
- neg_idx: int32 [16, 8, 2048], P(('sweep', 'ent')), parts along dimension 0
Outputs:
- output 1: float32 [65536, 200], P(('sweep', 'ent')), parts along dimension 0
- output 2: float32 [65536], P(('sweep', 'ent')), parts along dimension 0
- output 3: float32 [22, 200], P('sweep'), parts along dimension 0
- output 4: float32 [22], P('sweep'), parts along dimension 0
- output 5: float32 [16, 8], P(('sweep', 'ent')), parts along dimension 0
There are 2 independent parts. The reference program is written for one: setup_inputs(seed, part) draws one part's arguments, and reference() takes and returns one part's arrays. A program takes and returns all parts, laid end to end along the dimension named above; each array names one.
All inputs are finite; a program needn't handle non-finite values.
Results may differ from the reference program's by a relative error of at most 0.001.
Values are sent between devices in bfloat16 or wider.
A program may use at most 768 MiB of HBM per device.

```python
import jax
import jax.numpy as jnp
from jax import lax

GROUP_SIZE = 8
PART_ROWS = 4096
EMB_DIM = 200
NUM_RELS = 11
BUCKET_EDGES = 2048
NUM_NEGS = 2048
LR_ENT = 0.03
LR_REL = 0.05
ADA_EPS = 1e-10
HOT_ROWS = PART_ROWS // 16
HOT_RELS = max(NUM_RELS // 8, 1)


def draw_indices(index_key):
    sub_keys = jax.random.split(index_key, 12)
    edge_shape = (GROUP_SIZE, GROUP_SIZE, BUCKET_EDGES)

    def skewed(key_a, key_b, key_c, hot_odds, hot_count, full_count):
        pick_hot = jax.random.randint(key_a, edge_shape, 0, hot_odds) == 0
        hot_ids = jax.random.randint(key_b, edge_shape, 0, hot_count)
        all_ids = jax.random.randint(key_c, edge_shape, 0, full_count)
        return jnp.where(pick_hot, hot_ids, all_ids).astype(jnp.int32)

    head_idx = skewed(sub_keys[0], sub_keys[1], sub_keys[2], 4, HOT_ROWS, PART_ROWS)
    tail_idx = skewed(sub_keys[3], sub_keys[4], sub_keys[5], 4, HOT_ROWS, PART_ROWS)
    rel_idx = skewed(sub_keys[6], sub_keys[7], sub_keys[8], 2, HOT_RELS, NUM_RELS)
    fill_count = jax.random.randint(sub_keys[9], (GROUP_SIZE, GROUP_SIZE, 1), BUCKET_EDGES // 8, BUCKET_EDGES + 1)
    slot_draw = jax.random.randint(sub_keys[10], edge_shape, 0, BUCKET_EDGES)
    edge_mask = (slot_draw < fill_count).astype(jnp.int32)
    neg_idx = jax.random.randint(sub_keys[11], (GROUP_SIZE, GROUP_SIZE, NUM_NEGS), 0, PART_ROWS).astype(jnp.int32)
    return head_idx, tail_idx, rel_idx, edge_mask, neg_idx


def setup_inputs(seed: int = 0, part: int = 0) -> dict:
    part_key = jax.random.fold_in(jax.random.key(seed), part)
    sub_keys = jax.random.split(part_key, 5)
    total_rows = GROUP_SIZE * PART_ROWS
    ent_sigma = 1.2 * EMB_DIM ** -0.25
    ent_table = ent_sigma * jax.random.normal(sub_keys[0], (total_rows, EMB_DIM), jnp.float32)
    ent_scale = ent_sigma * ent_sigma * (BUCKET_EDGES / PART_ROWS + 1.0)
    ent_accum = ent_scale * jax.random.uniform(sub_keys[1], (total_rows,), jnp.float32, 0.2, 1.0)
    rel_table = 0.7071 * jax.random.normal(sub_keys[2], (NUM_RELS, EMB_DIM), jnp.float32)
    rel_scale = GROUP_SIZE * BUCKET_EDGES / (NUM_RELS * EMB_DIM)
    rel_accum = rel_scale * jax.random.uniform(sub_keys[3], (NUM_RELS,), jnp.float32, 0.3, 1.5)
    head_idx, tail_idx, rel_idx, edge_mask, neg_idx = draw_indices(sub_keys[4])
    return {"ent_table": ent_table, "ent_accum": ent_accum, "rel_table": rel_table, "rel_accum": rel_accum, "head_idx": head_idx, "tail_idx": tail_idx, "rel_idx": rel_idx, "edge_mask": edge_mask, "neg_idx": neg_idx}


def complex_mul(left_op, right_op):
    half_dim = left_op.shape[-1] // 2
    left_re, left_im = left_op[..., :half_dim], left_op[..., half_dim:]
    right_re, right_im = right_op[..., :half_dim], right_op[..., half_dim:]
    return jnp.concatenate([left_re * right_re - left_im * right_im, left_re * right_im + left_im * right_re], axis=-1)


def conj_mul(grad_in, other_op):
    half_dim = grad_in.shape[-1] // 2
    grad_re, grad_im = grad_in[..., :half_dim], grad_in[..., half_dim:]
    other_re, other_im = other_op[..., :half_dim], other_op[..., half_dim:]
    return jnp.concatenate([grad_re * other_re + grad_im * other_im, grad_im * other_re - grad_re * other_im], axis=-1)


def adagrad(param_rows, accum_rows, grad_rows, step_rate):
    new_accum = accum_rows + jnp.mean(grad_rows * grad_rows, axis=1)
    new_param = param_rows - step_rate * grad_rows / jnp.sqrt(new_accum + ADA_EPS)[:, None]
    return new_param, new_accum


def bucket_grads(head_rows, rel_rows, tail_rows, neg_rows, edge_w):
    query_bf = complex_mul(head_rows, rel_rows).astype(jnp.bfloat16)
    query_f32 = query_bf.astype(jnp.float32)
    tail_f32 = tail_rows.astype(jnp.float32)
    pos_score = jnp.sum(query_f32 * tail_f32, axis=1)
    neg_score = jnp.dot(query_bf, neg_rows.T, preferred_element_type=jnp.float32)
    logits = jnp.concatenate([pos_score[:, None], neg_score], axis=1)
    log_norm = jax.nn.logsumexp(logits, axis=1)
    weight = edge_w.astype(jnp.float32)
    round_loss = jnp.sum(weight * (log_norm - pos_score)) / edge_w.shape[0]
    soft_w = jnp.exp(logits - log_norm[:, None])
    d_pos = weight * (soft_w[:, 0] - 1.0)
    d_neg = (weight[:, None] * soft_w[:, 1:]).astype(jnp.bfloat16)
    d_query = d_pos[:, None] * tail_f32 + jnp.dot(d_neg, neg_rows, preferred_element_type=jnp.float32)
    d_negrows = jnp.dot(d_neg.T, query_bf, preferred_element_type=jnp.float32)
    d_tail = d_pos[:, None] * query_f32
    d_head = conj_mul(d_query, rel_rows)
    d_rel = conj_mul(d_query, head_rows)
    return d_head, d_tail, d_negrows, d_rel, round_loss


def reference(ent_table, ent_accum, rel_table, rel_accum, head_idx, tail_idx, rel_idx, edge_mask, neg_idx):
    total_rows = ent_table.shape[0]
    dev_ids = jnp.arange(GROUP_SIZE)
    head_base = dev_ids * PART_ROWS

    def train_step(carried, shift):
        cur_table, cur_accum, cur_rel, rel_acc = carried
        tail_base = ((dev_ids + shift) % GROUP_SIZE) * PART_ROWS
        heads_glob = head_base[:, None] + head_idx[:, shift]
        tails_glob = tail_base[:, None] + tail_idx[:, shift]
        negs_glob = tail_base[:, None] + neg_idx[:, shift]
        rels_now = rel_idx[:, shift]

        def per_device(bucket_in):
            heads_one, tails_one, negs_one, rels_one, mask_one = bucket_in
            head_rows = jnp.take(cur_table, heads_one, axis=0)
            rel_rows = jnp.take(cur_rel, rels_one, axis=0)
            tail_rows = jnp.take(cur_table, tails_one, axis=0).astype(jnp.bfloat16)
            neg_rows = jnp.take(cur_table, negs_one, axis=0).astype(jnp.bfloat16)
            return bucket_grads(head_rows, rel_rows, tail_rows, neg_rows, mask_one)

        d_head, d_tail, d_negrows, d_rel, round_loss = lax.map(per_device, (heads_glob, tails_glob, negs_glob, rels_now, edge_mask[:, shift]))
        row_grad = (jax.ops.segment_sum(d_head.reshape(-1, EMB_DIM), heads_glob.reshape(-1), num_segments=total_rows)
                    + jax.ops.segment_sum(d_tail.reshape(-1, EMB_DIM), tails_glob.reshape(-1), num_segments=total_rows)
                    + jax.ops.segment_sum(d_negrows.reshape(-1, EMB_DIM), negs_glob.reshape(-1), num_segments=total_rows))
        rel_grad = jax.ops.segment_sum(d_rel.reshape(-1, EMB_DIM), rels_now.reshape(-1), num_segments=NUM_RELS)
        new_table, new_accum = adagrad(cur_table, cur_accum, row_grad, LR_ENT)
        new_rel, new_racc = adagrad(cur_rel, rel_acc, rel_grad, LR_REL)
        return (new_table, new_accum, new_rel, new_racc), round_loss

    final_state, loss_rows = lax.scan(train_step, (ent_table, ent_accum, rel_table, rel_accum), jnp.arange(GROUP_SIZE))
    return final_state[0], final_state[1], final_state[2], final_state[3], loss_rows.T
```

```python
import functools

import jax
import jax.numpy as jnp
from jax import lax
from jax.experimental import pallas as pl
from jax.experimental.pallas import tpu as pltpu
from jax.sharding import PartitionSpec as P

LR_ENT = 0.03
LR_REL = 0.05
ADA_EPS = 1e-10
LANES = 128
MIB = 1024 * 1024
F32 = jnp.float32
BF16 = jnp.bfloat16
MESH = pl.DeviceIdType.MESH
VMEM = pl.BlockSpec(memory_space=pltpu.VMEM)
SMEM = pl.BlockSpec(memory_space=pltpu.SMEM)


def even(start, size):
    return pl.ds(start, size, stride=2)


def row_pair(index):
    return pl.ds(pl.multiple_of(index, 2), 2)


def transpose_row(row, width):
    return jnp.transpose(jnp.broadcast_to(row, (LANES, width)))


def gather_rows(count, streams, unroll=8):
    def body(step, carry):
        for sub in range(unroll):
            slot = step * unroll + sub
            for index_of, src, dst in streams:
                dst[row_pair(2 * slot), :] = src[row_pair(index_of(slot)), :]
        return carry

    lax.fori_loop(0, count // unroll, body, 0)


def scatter_rows(count, streams, unroll=4):
    def body(step, carry):
        for sub in range(unroll):
            slot = step * unroll + sub
            for index_of, src, table in streams:
                where = row_pair(index_of(slot))
                table[where, :] = table[where, :] + src[row_pair(2 * slot), :]
        return carry

    lax.fori_loop(0, count // unroll, body, 0)


def rel_exchange(group, part_ref, recv_ref, send_sem, recv_sem):
    me = lax.axis_index("ent")
    barrier = pltpu.get_barrier_semaphore()
    for off in range(1, group):
        pl.semaphore_signal(barrier, inc=1, device_id={"ent": lax.rem(me + off, group)}, device_id_type=MESH)
    pl.semaphore_wait(barrier, group - 1)
    copies = []
    for off in range(1, group):
        copy = pltpu.make_async_remote_copy(
            src_ref=part_ref,
            dst_ref=recv_ref.at[off],
            send_sem=send_sem.at[off],
            recv_sem=recv_sem.at[off],
            device_id={"ent": lax.rem(me + off, group)},
            device_id_type=MESH,
        )
        copy.start()
        copies.append(copy)

    def wait():
        for copy in copies:
            copy.wait()
        total = None
        for dev in range(group):
            off = lax.rem(me - dev + group, group)
            term = jnp.where(off == 0, part_ref[...], recv_ref[off])
            total = term if total is None else total + term
        return total

    return wait


def rel_update(total, rel, racc, dim):
    acc = racc + jnp.sum(total * total, axis=1, keepdims=True) * (1.0 / dim)
    scale = LR_REL * lax.rsqrt(acc + ADA_EPS)
    return rel - total * scale[:, :1], acc


def query_kernel(shift, ent, rel, own_idx, tail_idx, q_out, neg_out, tail_out, head_out, relrow_out, rel_pairs, buf_neg, buf_tail):
    count = q_out.shape[0]
    rels = rel.shape[0]
    gather_rows(count, [
        (lambda b: own_idx[shift, 0, b], ent, head_out),
        (lambda b: tail_idx[0, b], ent, buf_tail),
        (lambda b: tail_idx[1, b], ent, buf_neg),
    ])
    rel_pairs[even(0, rels), :] = rel[:, :LANES]
    rel_pairs[even(1, rels), :] = rel[:, LANES:]
    gather_rows(count, [(lambda b: own_idx[shift, 1, b], rel_pairs, relrow_out)])
    block = 128

    def body(step, carry):
        base = pl.multiple_of(step * block, block)
        rows = pl.ds(base, block)
        for src, dst in ((buf_neg, neg_out), (buf_tail, tail_out)):
            dst[rows, :LANES] = src[even(2 * base, block), :].astype(BF16)
            dst[rows, LANES:] = src[even(2 * base + 1, block), :].astype(BF16)
        head_re, head_im = head_out[even(2 * base, block), :], head_out[even(2 * base + 1, block), :]
        rel_re, rel_im = relrow_out[even(2 * base, block), :], relrow_out[even(2 * base + 1, block), :]
        q_out[rows, :LANES] = (head_re * rel_re - head_im * rel_im).astype(BF16)
        q_out[rows, LANES:] = (head_re * rel_im + head_im * rel_re).astype(BF16)
        return carry

    lax.fori_loop(0, count // block, body, 0)


def score_kernel(half, q, neg, tail, idx, dq_out, dneg_out, dtail_out, neg_t, score, attn):
    count, negs = q.shape[0], neg.shape[0]
    width = 256
    keep = dq_out.shape[0] // 2
    block = 128

    def flip(step, carry):
        cols = pl.ds(pl.multiple_of(step * width, width), width)
        neg_t[:, cols] = jnp.transpose(neg[cols, :].astype(F32)).astype(BF16)
        return carry

    lax.fori_loop(0, negs // width, flip, 0)

    def chunk(step, carry):
        base = pl.multiple_of(step * width, width)
        cols = pl.ds(base, width)
        q_now = q[cols, :]
        q_f32 = q_now.astype(F32)
        tail_f32 = tail[cols, :].astype(F32)
        score[...] = lax.dot_general(neg[...], q_now, (((1,), (1,)), ((), ())), preferred_element_type=F32)
        pos_col = jnp.sum(q_f32 * tail_f32, axis=1, keepdims=True)
        pos = jnp.transpose(jnp.broadcast_to(pos_col, (width, LANES)))[0:1, :]

        def top(k, best):
            part = score[pl.ds(pl.multiple_of(k * block, block), block), :]
            return jnp.maximum(best, jnp.max(part.reshape(block // 8, 8, width), axis=0))

        best = lax.fori_loop(0, negs // block, top, jnp.broadcast_to(pos, (8, width)))
        peak = jnp.max(best, axis=0, keepdims=True)

        def expo(k, acc):
            rows = pl.ds(pl.multiple_of(k * block, block), block)
            part = jnp.exp(score[rows, :] - peak)
            score[rows, :] = part
            return acc + jnp.sum(part.reshape(block // 8, 8, width), axis=0)

        acc = lax.fori_loop(0, negs // block, expo, jnp.zeros((8, width), F32))
        pos_exp = jnp.exp(pos - peak)
        norm = jnp.sum(acc, axis=0, keepdims=True) + pos_exp
        weight = idx[2:3, cols].astype(F32)
        inv = 1.0 / norm
        loss = weight * (peak + jnp.log(norm) - pos)
        d_pos = weight * (pos_exp * inv - 1.0)
        scale = weight * inv

        def scaled(k, carry):
            rows = pl.ds(pl.multiple_of(k * block, block), block)
            attn[rows, cols] = (score[rows, :] * scale).astype(BF16)
            return carry

        lax.fori_loop(0, negs // block, scaled, 0)
        d_q = jnp.dot(neg_t[...], attn[:, cols], preferred_element_type=F32) + d_pos * jnp.transpose(tail_f32)
        line = lax.broadcasted_iota(jnp.int32, (keep, width), 0)
        dq_out[:keep, cols] = d_q[:keep] + jnp.where(line == half, loss, 0.0)
        dq_out[keep:, cols] = d_q[LANES:LANES + keep]
        d_col = transpose_row(d_pos, width)
        dtail_out[even(2 * base, width), :] = d_col * q_f32[:, :LANES]
        dtail_out[even(2 * base + 1, width), :] = d_col * q_f32[:, LANES:]
        return carry

    lax.fori_loop(0, count // width, chunk, 0)
    rows_per = 512

    def back(step, carry):
        base = pl.multiple_of(step * rows_per, rows_per)
        got = jnp.dot(attn[pl.ds(base, rows_per), :], q[...], preferred_element_type=F32)
        dneg_out[even(2 * base, rows_per), :] = got[:, :LANES]
        dneg_out[even(2 * base + 1, rows_per), :] = got[:, LANES:]
        return carry

    lax.fori_loop(0, negs // rows_per, back, 0)


def split3(value):
    first = value.astype(BF16)
    rest = value - first.astype(F32)
    second = rest.astype(BF16)
    return first, second, (rest - second.astype(F32)).astype(BF16)


def update_kernel(dim, shift, ent, acc, dneg, dtail, dq, head, relrow, own_idx, own_vec, tail_idx, ent_out, acc_out, part_out, loss_out,
                  table_a, table_b, table_c, dhead):
    count = dhead.shape[0] // 2
    half = dim // 2
    keep = dq.shape[0] // 2
    rows_all = ent.shape[0]
    rels = part_out.shape[0]
    block = 128

    def zero(step, carry):
        rows = pl.ds(pl.multiple_of(step * 256, 256), 256)
        for table in (table_a, table_b, table_c):
            table[rows, :] = jnp.zeros((256, LANES), F32)
        return carry

    lax.fori_loop(0, rows_all // 256, zero, 0)
    loss_out[...] = jnp.broadcast_to(jnp.sum(dq[half:half + 1, :]) * (1.0 / count), loss_out.shape)
    part_out[...] = jnp.zeros(part_out.shape, F32)

    def heads(step, carry):
        base = pl.multiple_of(step * block, block)
        cols = pl.ds(base, block)
        line = lax.broadcasted_iota(jnp.int32, (keep, block), 0)
        pad = jnp.zeros((LANES - keep, block), F32)
        d_re = jnp.transpose(jnp.concatenate([jnp.where(line < half, dq[:keep, cols], 0.0), pad], axis=0))
        d_im = jnp.transpose(jnp.concatenate([dq[keep:, cols], pad], axis=0))
        rel_re, rel_im = relrow[even(2 * base, block), :], relrow[even(2 * base + 1, block), :]
        dhead[even(2 * base, block), :] = d_re * rel_re + d_im * rel_im
        dhead[even(2 * base + 1, block), :] = d_im * rel_re - d_re * rel_im
        head_re, head_im = head[even(2 * base, block), :], head[even(2 * base + 1, block), :]
        drel = jnp.concatenate([d_re * head_re + d_im * head_im, d_im * head_re - d_re * head_im], axis=1)
        pick = lax.broadcasted_iota(jnp.int32, (rels, block), 0) == own_vec[shift, 1:2, cols]
        hot = jnp.where(pick, 1.0, 0.0).astype(BF16)
        total = part_out[...]
        for piece in split3(drel):
            total = total + jnp.dot(hot, piece, preferred_element_type=F32)
        part_out[...] = total
        return carry

    lax.fori_loop(0, count // block, heads, 0)
    scatter_rows(count, [
        (lambda b: own_idx[shift, 0, b], dhead, table_a),
        (lambda b: tail_idx[0, b], dtail, table_b),
        (lambda b: tail_idx[1, b], dneg, table_c),
    ])

    def step_rows(step, carry):
        base = pl.multiple_of(step * block, block)
        rows = pl.ds(base, block)
        lo, hi = even(2 * base, block), even(2 * base + 1, block)
        g_re = table_a[lo, :] + (table_b[lo, :] + table_c[lo, :])
        g_im = table_a[hi, :] + (table_b[hi, :] + table_c[hi, :])
        new_acc = acc[rows, :] + jnp.sum(g_re * g_re + g_im * g_im, axis=1, keepdims=True) * (1.0 / dim)
        acc_out[rows, :] = new_acc
        scale = LR_ENT * lax.rsqrt(new_acc + ADA_EPS)
        ent_out[lo, :] = ent[lo, :] - g_re * scale
        ent_out[hi, :] = ent[hi, :] - g_im * scale
        return carry

    lax.fori_loop(0, rows_all // 2 // block, step_rows, 0)


def rel_kernel(group, dim, part, rel, racc, rel_out, racc_out, recv, send_sem, recv_sem):
    total = rel_exchange(group, part, recv, send_sem, recv_sem)()
    new_rel, new_acc = rel_update(total, rel[...], racc[...], dim)
    rel_out[...] = new_rel
    racc_out[...] = new_acc


def solution(mesh):
    group = mesh.shape["ent"]
    row_spec = P(("sweep", "ent"))
    table_spec = P(("sweep", "ent"), None)
    edge_spec = P(("sweep", "ent"), None, None)
    rel_spec = P("sweep", None)
    racc_spec = P("sweep")

    def device_step(ent_table, ent_accum, rel_table, rel_accum, head_idx, tail_idx, rel_idx, edge_mask, neg_idx):
        rows, dim = ent_table.shape
        half = dim // 2
        num_rels = rel_table.shape[0]
        rounds, count = head_idx.shape[1:]
        negs = neg_idx.shape[2]
        rels = -(-num_rels // 8) * 8
        keep = -(-(half + 1) // 8) * 8

        def spread(table):
            return jnp.pad(table.reshape(table.shape[0], 2, half), ((0, 0), (0, 0), (0, LANES - half)))

        ent = spread(ent_table).reshape(2 * rows, LANES)
        acc = jnp.broadcast_to(ent_accum[:, None], (rows, LANES))
        rel = jnp.pad(spread(rel_table).reshape(num_rels, 2 * LANES), ((0, rels - num_rels), (0, 0)))
        racc = jnp.broadcast_to(jnp.pad(rel_accum, (0, rels - num_rels))[:, None], (rels, LANES))
        own = jnp.stack([head_idx[0] * 2, rel_idx[0] * 2], axis=1)
        own_rel = jnp.stack([head_idx[0], rel_idx[0]], axis=1)
        away = jnp.stack([tail_idx[0] * 2, neg_idx[0] * 2, edge_mask[0]], axis=1)

        def shape(*dims, dtype=F32):
            return jax.ShapeDtypeStruct(dims, dtype)

        losses = []
        for shift in range(rounds):
            there = [(dev, (dev + shift) % group) for dev in range(group)]
            back = [(dst, src) for src, dst in there]
            incoming = away[shift] if shift == 0 else lax.ppermute(away[shift], "ent", there)
            scratch = [pltpu.VMEM((2 * rels, LANES), F32), pltpu.VMEM((2 * negs, LANES), F32), pltpu.VMEM((2 * count, LANES), F32)]
            q, neg, tail, head, relrow = pl.pallas_call(
                functools.partial(query_kernel, shift),
                out_shape=(shape(count, 2 * LANES, dtype=BF16), shape(negs, 2 * LANES, dtype=BF16), shape(count, 2 * LANES, dtype=BF16),
                           shape(2 * count, LANES), shape(2 * count, LANES)),
                in_specs=[VMEM, VMEM, SMEM, SMEM],
                out_specs=(VMEM,) * 5,
                scratch_shapes=scratch,
                compiler_params=pltpu.CompilerParams(vmem_limit_bytes=24 * MIB),
                name=f"query_{shift}",
            )(ent, rel, own, incoming)
            if shift:
                q = lax.ppermute(q, "ent", there)
            dq, dneg, dtail = pl.pallas_call(
                functools.partial(score_kernel, half),
                out_shape=(shape(2 * keep, count), shape(2 * negs, LANES), shape(2 * count, LANES)),
                in_specs=[VMEM] * 4,
                out_specs=(VMEM,) * 3,
                scratch_shapes=[pltpu.VMEM((2 * LANES, negs), BF16), pltpu.VMEM((negs, 256), F32), pltpu.VMEM((negs, count), BF16)],
                compiler_params=pltpu.CompilerParams(vmem_limit_bytes=32 * MIB),
                name="score",
            )(q, neg, tail, incoming)
            if shift:
                dq = lax.ppermute(dq, "ent", back)
            ent, acc, part, loss = pl.pallas_call(
                functools.partial(update_kernel, dim, shift),
                out_shape=(shape(2 * rows, LANES), shape(rows, LANES), shape(rels, 2 * LANES), shape(8, LANES)),
                in_specs=[VMEM] * 7 + [SMEM, VMEM, SMEM],
                out_specs=(VMEM,) * 4,
                scratch_shapes=[pltpu.VMEM((2 * rows, LANES), F32)] * 3 + [pltpu.VMEM((2 * count, LANES), F32)],
                input_output_aliases={0: 0, 1: 1},
                compiler_params=pltpu.CompilerParams(vmem_limit_bytes=46 * MIB),
                name=f"update_{shift}",
            )(ent, acc, dneg, dtail, dq, head, relrow, own, own_rel, incoming)
            losses.append(loss[0, 0])
            rel, racc = pl.pallas_call(
                functools.partial(rel_kernel, group, dim),
                out_shape=(shape(rels, 2 * LANES), shape(rels, LANES)),
                in_specs=[VMEM] * 3,
                out_specs=(VMEM,) * 2,
                scratch_shapes=[pltpu.VMEM((group, rels, 2 * LANES), F32), pltpu.SemaphoreType.DMA((group,)), pltpu.SemaphoreType.DMA((group,))],
                compiler_params=pltpu.CompilerParams(collective_id=0, has_side_effects=True, vmem_limit_bytes=4 * MIB),
                name="rel_step",
            )(part, rel, racc)
        new_ent = ent.reshape(rows, 2, LANES)[:, :, :half].reshape(rows, dim)
        new_rel = rel[:num_rels].reshape(num_rels, 2, LANES)[:, :, :half].reshape(num_rels, dim)
        return new_ent, acc[:, 0], new_rel, racc[:num_rels, 0], jnp.stack(losses)[None, :]

    return jax.shard_map(device_step, mesh=mesh, in_specs=(table_spec, row_spec, rel_spec, racc_spec, edge_spec, edge_spec, edge_spec, edge_spec, edge_spec), out_specs=(table_spec, row_spec, rel_spec, racc_spec, P(("sweep", "ent"), None)), check_vma=False)
```
